32 devices in a mesh: book: 4 (over y, core), path: 8 (over z, x).
Axes of the slice: x: 2, y: 2, z: 4, core: 2. Of those that a mesh axis runs over, the one named last changes fastest.
Arguments:
- states: float32 [10, 20, 65536], P(None, None, ('book', 'path')), parts along dimension 2, may hold values from -7.5 to 7.5
- itm_flags: int32 [10, 65536], P(None, ('book', 'path')), parts along dimension 1, may hold values 0 or 1
- terminal: float32 [65536], P(('book', 'path')), parts along dimension 0, may hold values from -3.5 to 5.5
- strike: float32 [4], P('book'), parts along dimension 0, may hold values from 0.025 to 0.035
- date_index: int32 [65536], P(('book', 'path')), parts along dimension 0, may hold values from 0 to 9
Outputs:
- cash_flow: float32 [65536], P(('book', 'path')), parts along dimension 0
- book_price: float32 [4], P('book'), parts along dimension 0
- coefficients: float32 [40, 231], P('book'), parts along dimension 0
The draws below stay inside these ranges and needn't reach their ends.
There are 4 independent parts, one for each index of `book`. The reference program is written for one: setup_inputs(seed, part) draws one part's arguments, and reference() takes and returns one part's arrays. A program takes and returns all parts, laid end to end along the dimension named above; each array names one. Nothing has to cross between parts.
All inputs are finite; a program needn't handle non-finite values. No bound on the sum of `itm_flags` on one device may be relied on, other than what follows from the above.
Results may differ from the reference program's by a relative error of at most 0.0003.
Values sent between devices are 32-bit elements; how exact they have to be, the bound alone decides.
A program may use at most 192 MiB of HBM per device.

```python
import jax
import jax.numpy as jnp
import numpy as np
from jax import lax

FACTORS = 20
DATES = 10
PATHS = 16384


def draw_states(key, part):
    position = (jnp.arange(PATHS, dtype=jnp.float32) + 0.5) / PATHS
    centre = 2.0 * position - 1.0
    spread = 0.5 * 3.0 ** position
    noise = jnp.clip(jax.random.normal(key, (DATES, FACTORS, PATHS), jnp.float32), -4.0, 4.0)
    offset = jnp.zeros((1, FACTORS, 1), jnp.float32)
    return centre + offset + spread * noise


def draw_terminal(key, part):
    position = (jnp.arange(PATHS, dtype=jnp.float32) + 0.5) / PATHS
    noise = jnp.clip(jax.random.normal(key, (PATHS,), jnp.float32), -4.0, 4.0)
    return 2.0 * position + 0.75 * noise


def set_ends(array, own_key, least, high):
    place = [jax.random.randint(jax.random.fold_in(own_key, axis), (), 0, length) for axis, length in enumerate(array.shape)]
    widest = array.shape.index(max(array.shape))
    beside = place[:widest] + [(place[widest] + 1) % array.shape[widest]] + place[widest + 1:]
    return array.at[tuple(place)].set(least).at[tuple(beside)].set(high)


def setup_inputs(seed: int = 0, part: int = 0) -> dict:
    key_list = jax.random.split(jax.random.key(seed), 6)
    part_splits = jax.random.split(jax.random.fold_in(key_list[5], part), 6)
    states = draw_states(jax.random.fold_in(jax.random.fold_in(key_list[5], part), 71), part)
    itm_flags = set_ends((jax.random.randint(part_splits[1], (DATES, PATHS), 0, 2) < 1).astype(jnp.int32), jax.random.fold_in(part_splits[1], 1), 0, 1)
    terminal = draw_terminal(jax.random.fold_in(jax.random.fold_in(key_list[5], part), 71), part)
    strike = jnp.clip(jax.random.uniform(part_splits[3], (1,), jnp.float32, 0.025, 0.035), 0.025, 0.035)
    date_index = set_ends(jax.random.randint(part_splits[4], (PATHS,), 0, DATES), jax.random.fold_in(part_splits[4], 1), 0, DATES - 1).astype(jnp.int32)
    return {"states": states, "itm_flags": itm_flags, "terminal": terminal, "strike": strike, "date_index": date_index}


ridge_weight = 0.05
temper_scale = 0.5
highest = lax.Precision.HIGHEST

def swap_terms(factors, strike_level):
    forwards = 0.03 * jnp.exp(0.25 * factors)
    discount = jnp.cumprod(1.0 / (1.0 + 0.25 * forwards), axis=0)
    annuity = 0.25 * lax.optimization_barrier(jnp.sum(discount, axis=0))
    swap_rate = (1.0 - discount[-1]) / annuity
    return (100.0 * annuity * (swap_rate - strike_level), discount[0])

def basis_of(scaled, pair_left, pair_right):
    ones_row = jnp.ones((1, scaled.shape[1]), scaled.dtype)
    return jnp.concatenate([ones_row, scaled, scaled[pair_left] * scaled[pair_right]], axis=0)

def solve_coefs(gram_sums, rhs_sums, path_count):
    system = gram_sums / path_count + ridge_weight * jnp.eye(gram_sums.shape[0], dtype=gram_sums.dtype)
    factor_chol = jnp.linalg.cholesky(system)
    return jax.scipy.linalg.cho_solve((factor_chol, True), rhs_sums / path_count)

def reference(states, itm_flags, terminal, strike, date_index):
    pair_left, pair_right = np.triu_indices(FACTORS)
    value_now = terminal
    coef_list = []
    for date_step in range(DATES - 1, -1, -1):
        factors = states[date_step]
        exercise, discount = swap_terms(factors, strike[0])
        value_now = value_now * discount
        money_flags = itm_flags[date_step].astype(jnp.float32)
        path_count = jnp.sum(money_flags)
        mean_vals = lax.optimization_barrier(jnp.sum(money_flags * factors, axis=1)) / path_count
        variance = lax.optimization_barrier(jnp.sum(money_flags * factors * factors, axis=1)) / path_count - mean_vals * mean_vals
        scale_vals = jnp.sqrt(variance + 1e-05)
        scaled = (factors - mean_vals[:, None]) / scale_vals[:, None]
        basis_rows = basis_of(scaled, pair_left, pair_right)
        weighted = basis_rows * money_flags
        gram_sums = lax.dot_general(weighted.astype(jnp.float32), basis_rows.astype(jnp.float32), (((1,), (1,)), ((), ())), precision=highest, preferred_element_type=jnp.float32)
        rhs_sums = jnp.dot(weighted.astype(jnp.float32), value_now.astype(jnp.float32), precision=highest, preferred_element_type=jnp.float32)
        coef_vector = solve_coefs(gram_sums, rhs_sums, path_count)
        continuation = jnp.dot(coef_vector.astype(jnp.float32), basis_rows.astype(jnp.float32), precision=highest, preferred_element_type=jnp.float32)
        open_date = (date_index <= date_step).astype(jnp.float32)
        weights = jax.nn.sigmoid((exercise - continuation) / temper_scale) * money_flags * open_date
        value_now = value_now + weights * (exercise - value_now)
        coef_list.append(coef_vector)
    book_price = jnp.reshape(jnp.sum(value_now) / PATHS, (1,))
    return (value_now, book_price, jnp.stack(coef_list[::-1], axis=0))
```

```python
import functools

import jax
import jax.numpy as jnp
from jax import lax
from jax.experimental import pallas as pl
from jax.experimental.pallas import tpu as pltpu
from jax.sharding import PartitionSpec as P

ridge_weight = 0.05
temper_scale = 0.5
highest = lax.Precision.HIGHEST
LANES = 128
BLOCK = 32
MESH = pl.DeviceIdType.MESH
VM = pl.BlockSpec(memory_space=pltpu.VMEM)


def round_up(n, k):
    return -(-n // k) * k


def peer(me, offset, n):
    return lax.rem(me + offset, n)


def entry_barrier(me, n):
    barrier = pltpu.get_barrier_semaphore()
    for o in range(1, n):
        pl.semaphore_signal(barrier, inc=1, device_id={"path": peer(me, o, n)}, device_id_type=MESH)
    pl.semaphore_wait(barrier, n - 1)


def column(stats, d):
    lane = lax.broadcasted_iota(jnp.int32, stats.shape, 1)
    return jnp.sum(jnp.where(lane == d, stats, 0.0), axis=1, keepdims=True)


def build_basis(z, mean, inv_scale, store):
    n = z.shape[0]
    x = (z - mean) * inv_scale
    store(0, jnp.ones((1, z.shape[1]), jnp.float32))
    store(1, x)
    at = 1 + n
    for j in range(n):
        store(at, x[j:j + 1] * x[j:])
        at += n - j
    return at


def stats_kernel(n, states, flags, out, mine, got, send_sem, recv_sem):
    me = lax.axis_index("path")
    dates, factors, _ = states.shape
    rows = round_up(factors, 8)
    lane = lax.broadcasted_iota(jnp.int32, (1, LANES), 1)
    first = jnp.zeros((factors, LANES), jnp.float32)
    second = jnp.zeros((factors, LANES), jnp.float32)
    count = jnp.zeros((1, LANES), jnp.float32)
    for d in range(dates):
        m = flags[d:d + 1, :].astype(jnp.float32)
        z = states[d]
        mz = m * z
        first = jnp.where(lane == d, jnp.sum(mz, axis=1, keepdims=True), first)
        second = jnp.where(lane == d, jnp.sum(mz * z, axis=1, keepdims=True), second)
        count = jnp.where(lane == d, jnp.sum(m, axis=1, keepdims=True), count)
    mine[...] = jnp.zeros_like(mine)
    mine[0:factors, :] = first
    mine[rows:rows + factors, :] = second
    mine[2 * rows:2 * rows + 1, :] = count
    entry_barrier(me, n)

    def copy(o):
        return pltpu.make_async_remote_copy(
            src_ref=mine, dst_ref=got.at[me], send_sem=send_sem.at[o], recv_sem=recv_sem.at[me],
            device_id={"path": peer(me, o, n)}, device_id_type=MESH)

    for o in range(1, n):
        copy(o).start()
    got[me] = mine[...]
    for o in range(1, n):
        p = peer(me, o, n)
        pltpu.make_async_remote_copy(
            src_ref=mine, dst_ref=got.at[p], send_sem=send_sem.at[o], recv_sem=recv_sem.at[p],
            device_id={"path": p}, device_id_type=MESH).wait_recv()
    total = got[0]
    for p in range(1, n):
        total = total + got[p]
    live = lane < dates
    count = jnp.where(live, total[2 * rows:2 * rows + 1], 1.0)
    mean = total[0:rows] / count
    variance = total[rows:2 * rows] / count - mean * mean
    scale = jnp.sqrt(jnp.where(live, variance, 0.0) + 1e-05)
    out[0:rows, :] = mean
    out[rows:2 * rows, :] = 1.0 / scale
    out[2 * rows:2 * rows + 8, :] = jnp.broadcast_to(count, (8, LANES))
    for o in range(1, n):
        copy(o).wait_send()


def gram_kernel(states, flags, stats, out, phi):
    d = pl.program_id(0)
    z = states[0]
    factors = z.shape[0]
    rows = round_up(factors, 8)
    m = flags[0].astype(jnp.float32)
    mean = column(stats[0:rows, :], d)[0:factors]
    inv_scale = column(stats[rows:2 * rows, :], d)[0:factors]
    size = phi.shape[0]

    def store(at, value):
        phi[at:at + value.shape[0], :] = value * m

    used = build_basis(z, mean, inv_scale, store)
    if used < size:
        phi[used:size, :] = jnp.zeros((size - used, z.shape[1]), jnp.float32)
    w = phi[...]
    hi = w.astype(jnp.bfloat16)
    rest = w - hi.astype(jnp.float32)
    mid = rest.astype(jnp.bfloat16)
    low = (rest - mid.astype(jnp.float32)).astype(jnp.bfloat16)

    def nt(a, b):
        return lax.dot_general(a, b, (((1,), (1,)), ((), ())), preferred_element_type=jnp.float32)

    cross = nt(hi, mid) + nt(hi, low)
    out[0] = (nt(hi, hi) + nt(mid, mid)) + (cross + cross.T)


def reduce_kernel(n, basis, grams, stats, out, got, send_sem, recv_sem):
    me = lax.axis_index("path")
    dates, size, _ = grams.shape
    slots = out.shape[0]
    count_row = stats.shape[0] - 8
    entry_barrier(me, n)

    def copy(e):
        owner, slot = e % n, e // n
        return pltpu.make_async_remote_copy(
            src_ref=grams.at[e], dst_ref=got.at[me, slot], send_sem=send_sem.at[e],
            recv_sem=recv_sem.at[me, slot], device_id={"path": owner}, device_id_type=MESH)

    for e in range(dates):
        @pl.when(me != e % n)
        def _():
            copy(e).start()
    ri = lax.broadcasted_iota(jnp.int32, (size, size), 0)
    ci = lax.broadcasted_iota(jnp.int32, (size, size), 1)
    for slot in range(slots):
        e = me + slot * n

        @pl.when(e < dates)
        def _():
            for o in range(1, n):
                p = peer(me, o, n)
                pltpu.make_async_remote_copy(
                    src_ref=grams.at[0], dst_ref=got.at[p, slot], send_sem=send_sem.at[0],
                    recv_sem=recv_sem.at[p, slot], device_id={"path": p}, device_id_type=MESH).wait_recv()
            total = grams[e]
            for o in range(1, n):
                total = total + got[peer(me, o, n), slot]
            count = column(stats[count_row:count_row + 8, :], e)[0:1]
            diag = jnp.where(ri < basis, ridge_weight, 1.0)
            out[slot] = total / count + jnp.where(ri == ci, diag, 0.0)

        @pl.when(e >= dates)
        def _():
            out[slot] = jnp.where(ri == ci, 1.0, 0.0)
    for e in range(dates):
        @pl.when(me != e % n)
        def _():
            copy(e).wait_send()


def small_inverse(d_list):
    b = d_list[0].shape[0]
    sub = lax.broadcasted_iota(jnp.int32, (b, b), 0)
    lane = lax.broadcasted_iota(jnp.int32, (b, b), 1)
    lane_row = lax.broadcasted_iota(jnp.int32, (1, b), 1)
    for j in range(b):
        new = []
        for d in d_list:
            inv = 1.0 / d[j:j + 1, j:j + 1]
            row = jnp.where(lane_row == j, inv, d[j:j + 1, :] * inv)
            col = d[:, j:j + 1]
            new.append(jnp.where(sub == j, row, jnp.where(lane == j, 0.0, d) - col * row))
        d_list = new
    return d_list


def inverse_kernel(system, out, work):
    slots, size, _ = system.shape
    work[...] = system[...]
    for k in range(size // BLOCK):
        lo, hi = k * BLOCK, (k + 1) * BLOCK
        diag = small_inverse([work[s, lo:hi, lo:hi] for s in range(slots)])
        for s in range(slots):
            rows = work[s, lo:hi, :]
            r = jnp.dot(diag[s], rows, precision=highest, preferred_element_type=jnp.float32)
            update = lax.dot_general(rows, r, (((0,), (0,)), ((), ())), precision=highest,
                                     preferred_element_type=jnp.float32)
            work[s] = work[s] - update
            work[s, lo:hi, :] = r
            work[s, :, lo:hi] = r.T
            work[s, lo:hi, lo:hi] = -diag[s]
    out[...] = -work[...]


def backward_kernel(n, states, flags, terminal, strike, date_index, stats, inverse,
                    flow, price, coefs,
                    phi, terms, inv_all, rhs_mine, rhs_got, sum_mine, sum_got,
                    inv_send, inv_recv, rhs_send, rhs_recv, sum_send, sum_recv):
    me = lax.axis_index("path")
    dates, factors, paths = states.shape
    size = phi.shape[1]
    rows = round_up(factors, 8)
    tiles = paths // LANES
    entry_barrier(me, n)

    def inv_copy(e, o):
        return pltpu.make_async_remote_copy(
            src_ref=inverse.at[e // n], dst_ref=inv_all.at[e], send_sem=inv_send.at[e, o],
            recv_sem=inv_recv.at[e], device_id={"path": peer(me, o, n)}, device_id_type=MESH)

    def own_copy(e):
        return pltpu.make_async_copy(inverse.at[e // n], inv_all.at[e], inv_recv.at[e])

    for e in range(dates - 1, -1, -1):
        @pl.when(me == e % n)
        def _():
            for o in range(1, n):
                inv_copy(e, o).start()
            own_copy(e).start()

    def prepare(d, slot):
        z = states[d]
        mean = column(stats[0:rows, :], d)[0:factors]
        inv_scale = column(stats[rows:2 * rows, :], d)[0:factors]

        def store(at, value):
            phi[slot, at:at + value.shape[0], :] = value

        used = build_basis(z, mean, inv_scale, store)
        if used < size:
            phi[slot, used:size, :] = jnp.zeros((size - used, paths), jnp.float32)
        step = 1.0 / (1.0 + 0.25 * (0.03 * jnp.exp(0.25 * z)))
        discount = step[0:1]
        total = discount
        for j in range(1, factors):
            discount = discount * step[j:j + 1]
            total = total + discount
        annuity = 0.25 * total
        swap_rate = (1.0 - discount) / annuity
        terms[slot, 0:1, :] = 100.0 * annuity * (swap_rate - strike[...])
        terms[slot, 1:2, :] = step[0:1]

    prepare(dates - 1, 0)
    coefs[...] = jnp.zeros_like(coefs)
    lane = lax.broadcasted_iota(jnp.int32, (1, LANES), 1)
    flow[...] = terminal[...]

    def rhs_copy(d, o):
        return pltpu.make_async_remote_copy(
            src_ref=rhs_mine.at[d], dst_ref=rhs_got.at[d, me], send_sem=rhs_send.at[d, o],
            recv_sem=rhs_recv.at[d, me], device_id={"path": peer(me, o, n)}, device_id_type=MESH)

    def step(i, carry):
        d = dates - 1 - i
        slot = lax.rem(i, 2)
        money = flags[pl.ds(d, 1), :].astype(jnp.float32)
        exercise = terms[slot, 0:1, :]
        value = flow[...] * terms[slot, 1:2, :]
        masked = value * money
        acc = jnp.zeros((size, LANES), jnp.float32)
        for t in range(tiles):
            cols = slice(t * LANES, (t + 1) * LANES)
            acc = acc + phi[slot, :, cols] * masked[:, cols]
        part = jnp.sum(acc.T.reshape(LANES // 8, 8, size), axis=0)
        rhs_mine[d] = part
        for o in range(1, n):
            rhs_copy(d, o).start()
        rhs_got[d, me] = part
        prepare(lax.max(d - 1, 0), 1 - slot)
        pltpu.make_async_copy(inverse.at[0], inv_all.at[d], inv_recv.at[d]).wait()
        for o in range(1, n):
            p = peer(me, o, n)
            pltpu.make_async_remote_copy(
                src_ref=rhs_mine.at[d], dst_ref=rhs_got.at[d, p], send_sem=rhs_send.at[d, o],
                recv_sem=rhs_recv.at[d, p], device_id={"path": p}, device_id_type=MESH).wait_recv()
        total = rhs_got[d, 0]
        for p in range(1, n):
            total = total + rhs_got[d, p]
        count = column(stats[2 * rows:2 * rows + 8, :], d)[0:1]
        rhs = jnp.sum(total, axis=0, keepdims=True) / count
        coef = jnp.sum(inv_all[d] * rhs, axis=1, keepdims=True)
        coefs[...] = jnp.where(lane == d, coef, coefs[...])
        coef_wide = jnp.broadcast_to(coef, (size, LANES))
        parts = []
        for t in range(tiles):
            cols = slice(t * LANES, (t + 1) * LANES)
            parts.append(jnp.sum(phi[slot, :, cols] * coef_wide, axis=0, keepdims=True))
        continuation = jnp.concatenate(parts, axis=1)
        open_date = jnp.where(date_index[...] <= d, money, 0.0)
        weights = jax.nn.sigmoid((exercise - continuation) / temper_scale) * open_date
        flow[...] = value + weights * (exercise - value)
        for o in range(1, n):
            rhs_copy(d, o).wait_send()
        return carry

    lax.fori_loop(0, dates, step, 0)

    final = flow[...]
    part = final[:, 0:LANES]
    for t in range(1, tiles):
        part = part + final[:, t * LANES:(t + 1) * LANES]
    wide = jnp.broadcast_to(part, (8, LANES))
    sum_mine[...] = wide

    def sum_copy(o):
        return pltpu.make_async_remote_copy(
            src_ref=sum_mine, dst_ref=sum_got.at[me], send_sem=sum_send.at[o],
            recv_sem=sum_recv.at[me], device_id={"path": peer(me, o, n)}, device_id_type=MESH)

    for o in range(1, n):
        sum_copy(o).start()
    sum_got[me] = wide
    for o in range(1, n):
        p = peer(me, o, n)
        pltpu.make_async_remote_copy(
            src_ref=sum_mine, dst_ref=sum_got.at[p], send_sem=sum_send.at[o],
            recv_sem=sum_recv.at[p], device_id={"path": p}, device_id_type=MESH).wait_recv()
    total = sum_got[0]
    for p in range(1, n):
        total = total + sum_got[p]
    price[...] = jnp.sum(total[0:1], axis=1, keepdims=True) / (paths * n)
    for o in range(1, n):
        sum_copy(o).wait_send()
    for e in range(dates):
        @pl.when(me == e % n)
        def _():
            for o in range(1, n):
                inv_copy(e, o).wait_send()


def shards(states, itm_flags, terminal, strike, date_index):
    n = lax.axis_size("path")
    dates, factors, paths = states.shape
    f32 = jnp.float32
    basis = 1 + factors + factors * (factors + 1) // 2
    size = round_up(basis, LANES)
    slots = -(-dates // n)
    rows = round_up(factors, 8)
    dma = pltpu.SemaphoreType.DMA
    big = 60 << 20

    def params(cid):
        return pltpu.CompilerParams(collective_id=cid, has_side_effects=True, vmem_limit_bytes=big)

    stats = pl.pallas_call(
        functools.partial(stats_kernel, n),
        out_shape=jax.ShapeDtypeStruct((2 * rows + 8, LANES), f32),
        in_specs=[VM, VM], out_specs=VM,
        scratch_shapes=[pltpu.VMEM((2 * rows + 8, LANES), f32),
                        pltpu.VMEM((n, 2 * rows + 8, LANES), f32), dma((n,)), dma((n,))],
        compiler_params=params(0), name="stats")(states, itm_flags)

    grams = pl.pallas_call(
        gram_kernel, grid=(dates,),
        out_shape=jax.ShapeDtypeStruct((dates, size, size), f32),
        in_specs=[pl.BlockSpec((1, factors, paths), lambda d: (d, 0, 0)),
                  pl.BlockSpec((1, 1, paths), lambda d: (d, 0, 0)),
                  VM],
        out_specs=pl.BlockSpec((1, size, size), lambda d: (d, 0, 0)),
        scratch_shapes=[pltpu.VMEM((size, paths), f32)],
        compiler_params=pltpu.CompilerParams(vmem_limit_bytes=big), name="gram",
    )(states, itm_flags[:, None, :], stats)

    system = pl.pallas_call(
        functools.partial(reduce_kernel, n, basis),
        out_shape=jax.ShapeDtypeStruct((slots, size, size), f32),
        in_specs=[VM, VM], out_specs=VM,
        scratch_shapes=[pltpu.VMEM((n, slots, size, size), f32), dma((dates,)), dma((n, slots))],
        compiler_params=params(1), name="reduce")(grams, stats)

    inverse = pl.pallas_call(
        inverse_kernel,
        out_shape=jax.ShapeDtypeStruct((slots, size, size), f32),
        in_specs=[VM], out_specs=VM,
        scratch_shapes=[pltpu.VMEM((slots, size, size), f32)],
        compiler_params=pltpu.CompilerParams(vmem_limit_bytes=big), name="inverse")(system)

    flow, price, coefs = pl.pallas_call(
        functools.partial(backward_kernel, n),
        out_shape=(jax.ShapeDtypeStruct((1, paths), f32), jax.ShapeDtypeStruct((1, 1), f32),
                   jax.ShapeDtypeStruct((size, LANES), f32)),
        in_specs=[VM] * 7, out_specs=(VM, VM, VM),
        scratch_shapes=[pltpu.VMEM((2, size, paths), f32), pltpu.VMEM((2, 8, paths), f32),
                        pltpu.VMEM((dates, size, size), f32),
                        pltpu.VMEM((dates, 8, size), f32), pltpu.VMEM((dates, n, 8, size), f32),
                        pltpu.VMEM((8, LANES), f32), pltpu.VMEM((n, 8, LANES), f32),
                        dma((dates, n)), dma((dates,)), dma((dates, n)), dma((dates, n)),
                        dma((n,)), dma((n,))],
        compiler_params=params(2), name="backward",
    )(states, itm_flags, terminal.reshape(1, paths), strike.reshape(1, 1),
      date_index.reshape(1, paths), stats, inverse)
    return flow.reshape(paths), price.reshape(1), coefs[:basis, :dates].T


def solution(mesh):
    in_specs = (
        P(None, None, ("book", "path")),
        P(None, ("book", "path")),
        P(("book", "path")),
        P("book"),
        P(("book", "path")),
    )
    out_specs = (P(("book", "path")), P("book"), P("book", None))
    return jax.shard_map(shards, mesh=mesh, in_specs=in_specs, out_specs=out_specs, check_vma=False)
```

```python
import functools

import jax
import jax.numpy as jnp
from jax import lax
from jax.experimental import pallas as pl
from jax.experimental.pallas import tpu as pltpu
from jax.sharding import PartitionSpec as P

ridge_weight = 0.05
temper_scale = 0.5
highest = lax.Precision.HIGHEST
LANES = 128
BLOCK = 32
MESH = pl.DeviceIdType.MESH
VM = pl.BlockSpec(memory_space=pltpu.VMEM)


def round_up(n, k):
    return -(-n // k) * k


def peer(me, offset, n):
    return lax.rem(me + offset, n)


def entry_barrier(me, n):
    barrier = pltpu.get_barrier_semaphore()
    for o in range(1, n):
        pl.semaphore_signal(barrier, inc=1, device_id={"path": peer(me, o, n)}, device_id_type=MESH)
    pl.semaphore_wait(barrier, n - 1)


def column(stats, d):
    lane = lax.broadcasted_iota(jnp.int32, stats.shape, 1)
    return jnp.sum(jnp.where(lane == d, stats, 0.0), axis=1, keepdims=True)


def build_basis(z, mean, inv_scale, store):
    n = z.shape[0]
    x = (z - mean) * inv_scale
    store(0, jnp.ones((1, z.shape[1]), jnp.float32))
    store(1, x)
    at = 1 + n
    for j in range(n):
        store(at, x[j:j + 1] * x[j:])
        at += n - j
    return at


def stats_kernel(n, states, flags, out, mine, got, send_sem, recv_sem):
    me = lax.axis_index("path")
    dates, factors, _ = states.shape
    rows = round_up(factors, 8)
    lane = lax.broadcasted_iota(jnp.int32, (1, LANES), 1)
    first = jnp.zeros((factors, LANES), jnp.float32)
    second = jnp.zeros((factors, LANES), jnp.float32)
    count = jnp.zeros((1, LANES), jnp.float32)
    for d in range(dates):
        m = flags[d:d + 1, :].astype(jnp.float32)
        z = states[d]
        mz = m * z
        first = jnp.where(lane == d, jnp.sum(mz, axis=1, keepdims=True), first)
        second = jnp.where(lane == d, jnp.sum(mz * z, axis=1, keepdims=True), second)
        count = jnp.where(lane == d, jnp.sum(m, axis=1, keepdims=True), count)
    mine[...] = jnp.zeros_like(mine)
    mine[0:factors, :] = first
    mine[rows:rows + factors, :] = second
    mine[2 * rows:2 * rows + 1, :] = count
    entry_barrier(me, n)

    def copy(o):
        return pltpu.make_async_remote_copy(
            src_ref=mine, dst_ref=got.at[me], send_sem=send_sem.at[o], recv_sem=recv_sem.at[me],
            device_id={"path": peer(me, o, n)}, device_id_type=MESH)

    for o in range(1, n):
        copy(o).start()
    got[me] = mine[...]
    for o in range(1, n):
        p = peer(me, o, n)
        pltpu.make_async_remote_copy(
            src_ref=mine, dst_ref=got.at[p], send_sem=send_sem.at[o], recv_sem=recv_sem.at[p],
            device_id={"path": p}, device_id_type=MESH).wait_recv()
    total = got[0]
    for p in range(1, n):
        total = total + got[p]
    live = lane < dates
    count = jnp.where(live, total[2 * rows:2 * rows + 1], 1.0)
    mean = total[0:rows] / count
    variance = total[rows:2 * rows] / count - mean * mean
    scale = jnp.sqrt(jnp.where(live, variance, 0.0) + 1e-05)
    out[0:rows, :] = mean
    out[rows:2 * rows, :] = 1.0 / scale
    out[2 * rows:2 * rows + 8, :] = jnp.broadcast_to(count, (8, LANES))
    for o in range(1, n):
        copy(o).wait_send()


def half_iotas():
    shape = (LANES, LANES)
    return lax.broadcasted_iota(jnp.int32, shape, 0), lax.broadcasted_iota(jnp.int32, shape, 1)


def fold(upper_left, lower_right):
    ri, ci = half_iotas()
    return jnp.where(ci <= ri, upper_left, pltpu.roll(lower_right, 1, 1))


def unfold(folded):
    ri, ci = half_iotas()
    shifted = pltpu.roll(folded, LANES - 1, 1)
    return (jnp.where(ci <= ri, folded, folded.T), jnp.where(ci >= ri, shifted, shifted.T))


def gram_kernel(n, basis, states, flags, stats, out, phi, packed, got, send_sem, recv_sem):
    me = lax.axis_index("path")
    dates, factors, paths = states.shape
    rows = round_up(factors, 8)
    size = phi.shape[0]
    slots = out.shape[0]
    height = packed.shape[1]
    entry_barrier(me, n)
    start = basis // 8 * 8
    phi[start:size, :] = jnp.zeros((size - start, paths), jnp.float32)

    def nt(a, b):
        return lax.dot_general(a, b, (((1,), (1,)), ((), ())), preferred_element_type=jnp.float32)

    def copy(e):
        return pltpu.make_async_remote_copy(
            src_ref=packed.at[e], dst_ref=got.at[me, e // n], send_sem=send_sem.at[e],
            recv_sem=recv_sem.at[me, e // n], device_id={"path": lax.rem(e, n)}, device_id_type=MESH)

    def step(d, carry):
        m = flags[pl.ds(d, 1), :].astype(jnp.float32)
        mean = column(stats[0:rows, :], d)[0:factors]
        inv_scale = column(stats[rows:2 * rows, :], d)[0:factors]

        def store(at, value):
            phi[at:at + value.shape[0], :] = value * m

        build_basis(states[d], mean, inv_scale, store)
        w = phi[...]
        hi = w.astype(jnp.bfloat16)
        rest = w - hi.astype(jnp.float32)
        mid = rest.astype(jnp.bfloat16)
        low = (rest - mid.astype(jnp.float32)).astype(jnp.bfloat16)
        cross = nt(hi, mid) + nt(hi, low)
        gram = (nt(hi, hi) + nt(mid, mid)) + (cross + cross.T)
        packed[d, 0:LANES, :] = fold(gram[0:LANES, 0:LANES], gram[LANES:, LANES:])
        packed[d, LANES:height, :] = gram[LANES:height, 0:LANES]

        @pl.when(me != lax.rem(d, n))
        def _():
            copy(d).start()
        return carry

    lax.fori_loop(0, dates, step, 0)
    ri = lax.broadcasted_iota(jnp.int32, (size, size), 0)
    ci = lax.broadcasted_iota(jnp.int32, (size, size), 1)
    for slot in range(slots):
        e = me + slot * n

        @pl.when(e < dates)
        def _():
            for o in range(1, n):
                p = peer(me, o, n)
                pltpu.make_async_remote_copy(
                    src_ref=packed.at[0], dst_ref=got.at[p, slot], send_sem=send_sem.at[0],
                    recv_sem=recv_sem.at[p, slot], device_id={"path": p}, device_id_type=MESH).wait_recv()
            total = packed[e]
            for o in range(1, n):
                total = total + got[peer(me, o, n), slot]
            first, last = unfold(total[0:LANES])
            below = jnp.concatenate(
                [total[LANES:], jnp.zeros((size - height, LANES), jnp.float32)], axis=0)
            full = jnp.concatenate([jnp.concatenate([first, below.T], axis=1),
                                    jnp.concatenate([below, last], axis=1)], axis=0)
            count = column(stats[2 * rows:2 * rows + 8, :], e)[0:1]
            full = jnp.where((ri < basis) & (ci < basis), full / count, 0.0)
            out[slot] = full + jnp.where(ri == ci, jnp.where(ri < basis, ridge_weight, 1.0), 0.0)

        @pl.when(e >= dates)
        def _():
            out[slot] = jnp.where(ri == ci, 1.0, 0.0)
    for e in range(dates):
        @pl.when(me != e % n)
        def _():
            copy(e).wait_send()


def small_inverse(d_list, live):
    b = d_list[0].shape[0]
    sub = lax.broadcasted_iota(jnp.int32, (b, b), 0)
    lane = lax.broadcasted_iota(jnp.int32, (b, b), 1)
    lane_row = lax.broadcasted_iota(jnp.int32, (1, b), 1)
    for j in range(live):
        new = []
        for d in d_list:
            inv = 1.0 / d[j:j + 1, j:j + 1]
            row = jnp.where(lane_row == j, inv, d[j:j + 1, :] * inv)
            col = d[:, j:j + 1]
            new.append(jnp.where(sub == j, row, jnp.where(lane == j, 0.0, d) - col * row))
        d_list = new
    return d_list


def inverse_kernel(basis, system, out, work):
    slots, size, _ = system.shape
    work[...] = system[...]
    for k in range(-(-basis // BLOCK)):
        lo, hi = k * BLOCK, (k + 1) * BLOCK
        diag = small_inverse([work[s, lo:hi, lo:hi] for s in range(slots)],
                             min(BLOCK, basis - lo))
        for s in range(slots):
            rows = work[s, lo:hi, :]
            r = jnp.dot(diag[s], rows, precision=highest, preferred_element_type=jnp.float32)
            update = lax.dot_general(rows, r, (((0,), (0,)), ((), ())), precision=highest,
                                     preferred_element_type=jnp.float32)
            work[s] = work[s] - update
            work[s, lo:hi, :] = r
            work[s, :, lo:hi] = r.T
            work[s, lo:hi, lo:hi] = -diag[s]
    height = out.shape[1]
    for s in range(slots):
        out[s, 0:LANES, :] = -fold(work[s, 0:LANES, 0:LANES], work[s, LANES:, LANES:])
        out[s, LANES:height, :] = -work[s, LANES:height, 0:LANES]


def backward_kernel(n, ahead, states, flags, terminal, strike, date_index, stats, inverse,
                    flow, price, coefs,
                    phi, terms, inv_all, inv_full, rhs_mine, rhs_got, sum_mine, sum_got,
                    inv_send, inv_recv, rhs_send, rhs_recv, sum_send, sum_recv):
    me = lax.axis_index("path")
    dates, factors, paths = states.shape
    size = phi.shape[1]
    rows = round_up(factors, 8)
    tiles = paths // LANES
    entry_barrier(me, n)

    def inv_copy(e, o):
        return pltpu.make_async_remote_copy(
            src_ref=inverse.at[e // n], dst_ref=inv_all.at[e], send_sem=inv_send.at[e, o],
            recv_sem=inv_recv.at[e], device_id={"path": peer(me, o, n)}, device_id_type=MESH)

    def own_copy(e):
        return pltpu.make_async_copy(inverse.at[e // n], inv_all.at[e], inv_recv.at[e])

    def send_inverse(e, live):
        @pl.when(live & (me == lax.rem(e, n)))
        def _():
            own_copy(e).start()
            for o in range(1, n):
                inv_copy(e, o).start()

    for e in range(dates - 1, dates - 1 - ahead, -1):
        send_inverse(e, me >= 0)
    inv_full[...] = jnp.zeros_like(inv_full)
    height = inv_all.shape[1]

    def prepare(d, slot):
        z = states[d]
        mean = column(stats[0:rows, :], d)[0:factors]
        inv_scale = column(stats[rows:2 * rows, :], d)[0:factors]

        def store(at, value):
            phi[slot, at:at + value.shape[0], :] = value

        used = build_basis(z, mean, inv_scale, store)
        if used < size:
            phi[slot, used:size, :] = jnp.zeros((size - used, paths), jnp.float32)
        step = 1.0 / (1.0 + 0.25 * (0.03 * jnp.exp(0.25 * z)))
        discount = step[0:1]
        total = discount
        for j in range(1, factors):
            discount = discount * step[j:j + 1]
            total = total + discount
        annuity = 0.25 * total
        swap_rate = (1.0 - discount) / annuity
        terms[slot, 0:1, :] = 100.0 * annuity * (swap_rate - strike[...])
        terms[slot, 1:2, :] = step[0:1]

    prepare(dates - 1, 0)
    coefs[...] = jnp.zeros_like(coefs)
    lane = lax.broadcasted_iota(jnp.int32, (1, LANES), 1)
    flow[...] = terminal[...]

    def rhs_copy(d, o):
        return pltpu.make_async_remote_copy(
            src_ref=rhs_mine.at[d], dst_ref=rhs_got.at[d, me], send_sem=rhs_send.at[d, o],
            recv_sem=rhs_recv.at[d, me], device_id={"path": peer(me, o, n)}, device_id_type=MESH)

    def step(i, carry):
        d = dates - 1 - i
        slot = lax.rem(i, 2)
        money = flags[pl.ds(d, 1), :].astype(jnp.float32)
        exercise = terms[slot, 0:1, :]
        value = flow[...] * terms[slot, 1:2, :]
        masked = value * money
        acc = jnp.zeros((size, LANES), jnp.float32)
        for t in range(tiles):
            cols = slice(t * LANES, (t + 1) * LANES)
            acc = acc + phi[slot, :, cols] * masked[:, cols]
        part = jnp.sum(acc.T.reshape(LANES // 8, 8, size), axis=0)
        rhs_mine[d] = part
        for o in range(1, n):
            rhs_copy(d, o).start()
        rhs_got[d, me] = part
        send_inverse(lax.max(d - ahead, 0), d >= ahead)
        prepare(lax.max(d - 1, 0), 1 - slot)
        pltpu.make_async_copy(inverse.at[0], inv_all.at[d], inv_recv.at[d]).wait()
        first, last = unfold(inv_all[d, 0:LANES, :])
        inv_full[0:LANES, 0:LANES] = first
        inv_full[LANES:, LANES:] = last
        inv_full[LANES:height, 0:LANES] = inv_all[d, LANES:height, :]
        inv_full[0:LANES, LANES:] = inv_full[LANES:, 0:LANES].T
        for o in range(1, n):
            p = peer(me, o, n)
            pltpu.make_async_remote_copy(
                src_ref=rhs_mine.at[d], dst_ref=rhs_got.at[d, p], send_sem=rhs_send.at[d, o],
                recv_sem=rhs_recv.at[d, p], device_id={"path": p}, device_id_type=MESH).wait_recv()
        total = rhs_got[d, 0]
        for p in range(1, n):
            total = total + rhs_got[d, p]
        count = column(stats[2 * rows:2 * rows + 8, :], d)[0:1]
        rhs = jnp.sum(total, axis=0, keepdims=True) / count
        coef = jnp.sum(inv_full[...] * rhs, axis=1, keepdims=True)
        coefs[...] = jnp.where(lane == d, coef, coefs[...])
        coef_wide = jnp.broadcast_to(coef, (size, LANES))
        parts = []
        for t in range(tiles):
            cols = slice(t * LANES, (t + 1) * LANES)
            parts.append(jnp.sum(phi[slot, :, cols] * coef_wide, axis=0, keepdims=True))
        continuation = jnp.concatenate(parts, axis=1)
        open_date = jnp.where(date_index[...] <= d, money, 0.0)
        weights = jax.nn.sigmoid((exercise - continuation) / temper_scale) * open_date
        flow[...] = value + weights * (exercise - value)
        for o in range(1, n):
            rhs_copy(d, o).wait_send()
        return carry

    lax.fori_loop(0, dates, step, 0)

    final = flow[...]
    part = final[:, 0:LANES]
    for t in range(1, tiles):
        part = part + final[:, t * LANES:(t + 1) * LANES]
    wide = jnp.broadcast_to(part, (8, LANES))
    sum_mine[...] = wide

    def sum_copy(o):
        return pltpu.make_async_remote_copy(
            src_ref=sum_mine, dst_ref=sum_got.at[me], send_sem=sum_send.at[o],
            recv_sem=sum_recv.at[me], device_id={"path": peer(me, o, n)}, device_id_type=MESH)

    for o in range(1, n):
        sum_copy(o).start()
    sum_got[me] = wide
    for o in range(1, n):
        p = peer(me, o, n)
        pltpu.make_async_remote_copy(
            src_ref=sum_mine, dst_ref=sum_got.at[p], send_sem=sum_send.at[o],
            recv_sem=sum_recv.at[p], device_id={"path": p}, device_id_type=MESH).wait_recv()
    total = sum_got[0]
    for p in range(1, n):
        total = total + sum_got[p]
    price[...] = jnp.sum(total[0:1], axis=1, keepdims=True) / (paths * n)
    for o in range(1, n):
        sum_copy(o).wait_send()
    for e in range(dates):
        @pl.when(me == e % n)
        def _():
            for o in range(1, n):
                inv_copy(e, o).wait_send()


def shards(states, itm_flags, terminal, strike, date_index):
    n = lax.axis_size("path")
    dates, factors, paths = states.shape
    f32 = jnp.float32
    basis = 1 + factors + factors * (factors + 1) // 2
    size = 2 * LANES
    height = round_up(basis, 8)
    assert LANES < basis < size
    slots = -(-dates // n)
    rows = round_up(factors, 8)
    dma = pltpu.SemaphoreType.DMA
    big = 60 << 20

    def params(cid):
        return pltpu.CompilerParams(collective_id=cid, has_side_effects=True, vmem_limit_bytes=big)

    stats = pl.pallas_call(
        functools.partial(stats_kernel, n),
        out_shape=jax.ShapeDtypeStruct((2 * rows + 8, LANES), f32),
        in_specs=[VM, VM], out_specs=VM,
        scratch_shapes=[pltpu.VMEM((2 * rows + 8, LANES), f32),
                        pltpu.VMEM((n, 2 * rows + 8, LANES), f32), dma((n,)), dma((n,))],
        compiler_params=params(0), name="stats")(states, itm_flags)

    system = pl.pallas_call(
        functools.partial(gram_kernel, n, basis),
        out_shape=jax.ShapeDtypeStruct((slots, size, size), f32),
        in_specs=[VM, VM, VM], out_specs=VM,
        scratch_shapes=[pltpu.VMEM((size, paths), f32), pltpu.VMEM((dates, height, LANES), f32),
                        pltpu.VMEM((n, slots, height, LANES), f32), dma((dates,)), dma((n, slots))],
        compiler_params=params(1), name="gram")(states, itm_flags, stats)

    inverse = pl.pallas_call(
        functools.partial(inverse_kernel, basis),
        out_shape=jax.ShapeDtypeStruct((slots, height, LANES), f32),
        in_specs=[VM], out_specs=VM,
        scratch_shapes=[pltpu.VMEM((slots, size, size), f32)],
        compiler_params=pltpu.CompilerParams(vmem_limit_bytes=big), name="inverse")(system)

    flow, price, coefs = pl.pallas_call(
        functools.partial(backward_kernel, n, min(3, dates)),
        out_shape=(jax.ShapeDtypeStruct((1, paths), f32), jax.ShapeDtypeStruct((1, 1), f32),
                   jax.ShapeDtypeStruct((size, LANES), f32)),
        in_specs=[VM] * 7, out_specs=(VM, VM, VM),
        scratch_shapes=[pltpu.VMEM((2, size, paths), f32), pltpu.VMEM((2, 8, paths), f32),
                        pltpu.VMEM((dates, height, LANES), f32), pltpu.VMEM((size, size), f32),
                        pltpu.VMEM((dates, 8, size), f32), pltpu.VMEM((dates, n, 8, size), f32),
                        pltpu.VMEM((8, LANES), f32), pltpu.VMEM((n, 8, LANES), f32),
                        dma((dates, n)), dma((dates,)), dma((dates, n)), dma((dates, n)),
                        dma((n,)), dma((n,))],
        compiler_params=params(2), name="backward",
    )(states, itm_flags, terminal.reshape(1, paths), strike.reshape(1, 1),
      date_index.reshape(1, paths), stats, inverse)
    return flow.reshape(paths), price.reshape(1), coefs[:basis, :dates].T


def solution(mesh):
    in_specs = (
        P(None, None, ("book", "path")),
        P(None, ("book", "path")),
        P(("book", "path")),
        P("book"),
        P(("book", "path")),
    )
    out_specs = (P(("book", "path")), P("book"), P("book", None))
    return jax.shard_map(shards, mesh=mesh, in_specs=in_specs, out_specs=out_specs, check_vma=False)
```

```python
import functools

import jax
import jax.numpy as jnp
from jax import lax
from jax.experimental import pallas as pl
from jax.experimental.pallas import tpu as pltpu
from jax.sharding import PartitionSpec as P

ridge_weight = 0.05
temper_scale = 0.5
highest = lax.Precision.HIGHEST
LANES = 128
BLOCK = LANES
MESH = pl.DeviceIdType.MESH
VM = pl.BlockSpec(memory_space=pltpu.VMEM)


def round_up(n, k):
    return -(-n // k) * k


def peer(me, offset, n):
    return lax.rem(me + offset, n)


def entry_barrier(me, n):
    barrier = pltpu.get_barrier_semaphore()
    for o in range(1, n):
        pl.semaphore_signal(barrier, inc=1, device_id={"path": peer(me, o, n)}, device_id_type=MESH)
    pl.semaphore_wait(barrier, n - 1)


def column(stats, d):
    lane = lax.broadcasted_iota(jnp.int32, stats.shape, 1)
    return jnp.sum(jnp.where(lane == d, stats, 0.0), axis=1, keepdims=True)


def build_basis(z, mean, inv_scale, store):
    n = z.shape[0]
    x = (z - mean) * inv_scale
    store(0, jnp.ones((1, z.shape[1]), jnp.float32))
    store(1, x)
    at = 1 + n
    for j in range(n):
        store(at, x[j:j + 1] * x[j:])
        at += n - j
    return at


def stats_kernel(n, states, flags, out, wide, mine, got, send_sem, recv_sem):
    me = lax.axis_index("path")
    dates, factors, _ = states.shape
    rows = round_up(factors, 8)
    lane = lax.broadcasted_iota(jnp.int32, (1, LANES), 1)
    first = jnp.zeros((factors, LANES), jnp.float32)
    second = jnp.zeros((factors, LANES), jnp.float32)
    count = jnp.zeros((1, LANES), jnp.float32)
    for d in range(dates):
        m = flags[d:d + 1, :].astype(jnp.float32)
        z = states[d]
        mz = m * z
        first = jnp.where(lane == d, jnp.sum(mz, axis=1, keepdims=True), first)
        second = jnp.where(lane == d, jnp.sum(mz * z, axis=1, keepdims=True), second)
        count = jnp.where(lane == d, jnp.sum(m, axis=1, keepdims=True), count)
    wide[...] = jnp.zeros_like(wide)
    wide[0:factors, :] = first
    wide[rows:rows + factors, :] = second
    wide[2 * rows:2 * rows + 1, :] = count
    mine[...] = wide[...].T[0:mine.shape[0]]
    entry_barrier(me, n)

    def copy(o):
        return pltpu.make_async_remote_copy(
            src_ref=mine, dst_ref=got.at[me], send_sem=send_sem.at[o], recv_sem=recv_sem.at[me],
            device_id={"path": peer(me, o, n)}, device_id_type=MESH)

    for o in range(1, n):
        copy(o).start()
    got[me] = mine[...]
    for o in range(1, n):
        p = peer(me, o, n)
        pltpu.make_async_remote_copy(
            src_ref=mine, dst_ref=got.at[p], send_sem=send_sem.at[o], recv_sem=recv_sem.at[p],
            device_id={"path": p}, device_id_type=MESH).wait_recv()
    total = got[0]
    for p in range(1, n):
        total = total + got[p]
    wide[0:total.shape[0], :] = total
    wide[total.shape[0]:, :] = jnp.zeros((LANES - total.shape[0], LANES), jnp.float32)
    total = wide[...].T
    live = lane < dates
    count = jnp.where(live, total[2 * rows:2 * rows + 1], 1.0)
    mean = total[0:rows] / count
    variance = total[rows:2 * rows] / count - mean * mean
    scale = jnp.sqrt(jnp.where(live, variance, 0.0) + 1e-05)
    out[0:rows, :] = mean
    out[rows:2 * rows, :] = 1.0 / scale
    out[2 * rows:2 * rows + 8, :] = jnp.broadcast_to(count, (8, LANES))
    for o in range(1, n):
        copy(o).wait_send()


def half_iotas():
    shape = (LANES, LANES)
    return lax.broadcasted_iota(jnp.int32, shape, 0), lax.broadcasted_iota(jnp.int32, shape, 1)


def fold(upper_left, lower_right):
    ri, ci = half_iotas()
    return jnp.where(ci <= ri, upper_left, pltpu.roll(lower_right, 1, 1))


def unfold(folded):
    ri, ci = half_iotas()
    shifted = pltpu.roll(folded, LANES - 1, 1)
    return (jnp.where(ci <= ri, folded, folded.T), jnp.where(ci >= ri, shifted, shifted.T))


def gram_kernel(n, basis, states, flags, stats, out, phi, packed, got, send_sem, recv_sem):
    me = lax.axis_index("path")
    dates, factors, paths = states.shape
    rows = round_up(factors, 8)
    size = phi.shape[0]
    slots = out.shape[0]
    height = packed.shape[1]
    entry_barrier(me, n)
    start = basis // 8 * 8
    phi[start:size, :] = jnp.zeros((size - start, paths), jnp.float32)

    def nt(a, b):
        return lax.dot_general(a, b, (((1,), (1,)), ((), ())), preferred_element_type=jnp.float32)

    def copy(e):
        return pltpu.make_async_remote_copy(
            src_ref=packed.at[e], dst_ref=got.at[me, e // n], send_sem=send_sem.at[e],
            recv_sem=recv_sem.at[me, e // n], device_id={"path": lax.rem(e, n)}, device_id_type=MESH)

    def step(d, carry):
        m = flags[pl.ds(d, 1), :].astype(jnp.float32)
        mean = column(stats[0:rows, :], d)[0:factors]
        inv_scale = column(stats[rows:2 * rows, :], d)[0:factors]

        def store(at, value):
            phi[at:at + value.shape[0], :] = value * m

        build_basis(states[d], mean, inv_scale, store)
        w = phi[...]
        hi = w.astype(jnp.bfloat16)
        rest = w - hi.astype(jnp.float32)
        mid = rest.astype(jnp.bfloat16)
        low = (rest - mid.astype(jnp.float32)).astype(jnp.bfloat16)
        cross = nt(hi, mid) + nt(hi, low)
        gram = (nt(hi, hi) + nt(mid, mid)) + (cross + cross.T)
        packed[d, 0:LANES, :] = fold(gram[0:LANES, 0:LANES], gram[LANES:, LANES:])
        packed[d, LANES:height, :] = gram[LANES:height, 0:LANES]

        @pl.when(me != lax.rem(d, n))
        def _():
            copy(d).start()
        return carry

    lax.fori_loop(0, dates, step, 0)
    ri = lax.broadcasted_iota(jnp.int32, (size, size), 0)
    ci = lax.broadcasted_iota(jnp.int32, (size, size), 1)
    for slot in range(slots):
        e = me + slot * n

        @pl.when(e < dates)
        def _():
            for o in range(1, n):
                p = peer(me, o, n)
                pltpu.make_async_remote_copy(
                    src_ref=packed.at[0], dst_ref=got.at[p, slot], send_sem=send_sem.at[0],
                    recv_sem=recv_sem.at[p, slot], device_id={"path": p}, device_id_type=MESH).wait_recv()
            total = packed[e]
            for o in range(1, n):
                total = total + got[peer(me, o, n), slot]
            first, last = unfold(total[0:LANES])
            below = jnp.concatenate(
                [total[LANES:], jnp.zeros((size - height, LANES), jnp.float32)], axis=0)
            full = jnp.concatenate([jnp.concatenate([first, below.T], axis=1),
                                    jnp.concatenate([below, last], axis=1)], axis=0)
            count = column(stats[2 * rows:2 * rows + 8, :], e)[0:1]
            full = jnp.where((ri < basis) & (ci < basis), full / count, 0.0)
            out[slot] = full + jnp.where(ri == ci, jnp.where(ri < basis, ridge_weight, 1.0), 0.0)

        @pl.when(e >= dates)
        def _():
            out[slot] = jnp.where(ri == ci, 1.0, 0.0)
    for e in range(dates):
        @pl.when(me != e % n)
        def _():
            copy(e).wait_send()


def small_inverse(d_list, live):
    b = d_list[0].shape[0]
    sub = lax.broadcasted_iota(jnp.int32, (b, b), 0)
    lane = lax.broadcasted_iota(jnp.int32, (b, b), 1)
    lane_row = lax.broadcasted_iota(jnp.int32, (1, b), 1)
    for j in range(live):
        new = []
        for d in d_list:
            inv = 1.0 / d[j:j + 1, j:j + 1]
            row = jnp.where(lane_row == j, inv, d[j:j + 1, :] * inv)
            col = d[:, j:j + 1]
            new.append(jnp.where(sub == j, row, jnp.where(lane == j, 0.0, d) - col * row))
        d_list = new
    return d_list


def inverse_kernel(basis, system, out, work):
    slots, size, _ = system.shape
    work[...] = system[...]
    for k in range(-(-basis // BLOCK)):
        lo, hi = k * BLOCK, (k + 1) * BLOCK
        diag = small_inverse([work[s, lo:hi, lo:hi] for s in range(slots)],
                             min(BLOCK, basis - lo))
        for s in range(slots):
            rows = work[s, lo:hi, :]
            r = jnp.dot(diag[s], rows, precision=highest, preferred_element_type=jnp.float32)
            update = lax.dot_general(rows, r, (((0,), (0,)), ((), ())), precision=highest,
                                     preferred_element_type=jnp.float32)
            work[s] = work[s] - update
            work[s, lo:hi, :] = r
            work[s, :, lo:hi] = r.T
            work[s, lo:hi, lo:hi] = -diag[s]
    height = out.shape[1]
    for s in range(slots):
        out[s, 0:LANES, :] = -fold(work[s, 0:LANES, 0:LANES], work[s, LANES:, LANES:])
        out[s, LANES:height, :] = -work[s, LANES:height, 0:LANES]


def backward_kernel(n, ahead, states, flags, terminal, strike, date_index, stats, inverse,
                    flow, price, coefs,
                    phi, terms, inv_all, inv_full, rhs_mine, rhs_got, sum_mine, sum_got,
                    inv_send, inv_recv, rhs_send, rhs_recv, sum_send, sum_recv):
    me = lax.axis_index("path")
    dates, factors, paths = states.shape
    size = phi.shape[1]
    rows = round_up(factors, 8)
    tiles = paths // LANES
    entry_barrier(me, n)

    def inv_copy(e, o):
        return pltpu.make_async_remote_copy(
            src_ref=inverse.at[e // n], dst_ref=inv_all.at[e], send_sem=inv_send.at[e, o],
            recv_sem=inv_recv.at[e], device_id={"path": peer(me, o, n)}, device_id_type=MESH)

    def own_copy(e):
        return pltpu.make_async_copy(inverse.at[e // n], inv_all.at[e], inv_recv.at[e])

    def send_inverse(e, live):
        @pl.when(live & (me == lax.rem(e, n)))
        def _():
            own_copy(e).start()
            for o in range(1, n):
                inv_copy(e, o).start()

    for e in range(dates - 1, dates - 1 - ahead, -1):
        send_inverse(e, me >= 0)
    inv_full[...] = jnp.zeros_like(inv_full)
    height = inv_all.shape[1]

    def prepare(d, slot):
        z = states[d]
        mean = column(stats[0:rows, :], d)[0:factors]
        inv_scale = column(stats[rows:2 * rows, :], d)[0:factors]

        def store(at, value):
            phi[slot, at:at + value.shape[0], :] = value

        used = build_basis(z, mean, inv_scale, store)
        if used < size:
            phi[slot, used:size, :] = jnp.zeros((size - used, paths), jnp.float32)
        step = 1.0 / (1.0 + 0.25 * (0.03 * jnp.exp(0.25 * z)))
        discount = step[0:1]
        total = discount
        for j in range(1, factors):
            discount = discount * step[j:j + 1]
            total = total + discount
        annuity = 0.25 * total
        swap_rate = (1.0 - discount) / annuity
        terms[slot, 0:1, :] = 100.0 * annuity * (swap_rate - strike[...])
        terms[slot, 1:2, :] = step[0:1]

    prepare(dates - 1, 0)
    coefs[...] = jnp.zeros_like(coefs)
    lane = lax.broadcasted_iota(jnp.int32, (1, LANES), 1)
    flow[...] = terminal[...]

    def rhs_copy(d, o):
        return pltpu.make_async_remote_copy(
            src_ref=rhs_mine.at[d], dst_ref=rhs_got.at[d, me], send_sem=rhs_send.at[d, o],
            recv_sem=rhs_recv.at[d, me], device_id={"path": peer(me, o, n)}, device_id_type=MESH)

    def step(i, carry):
        d = dates - 1 - i
        slot = lax.rem(i, 2)
        money = flags[pl.ds(d, 1), :].astype(jnp.float32)
        exercise = terms[slot, 0:1, :]
        value = flow[...] * terms[slot, 1:2, :]
        masked = value * money
        acc = jnp.zeros((size, LANES), jnp.float32)
        for t in range(tiles):
            cols = slice(t * LANES, (t + 1) * LANES)
            acc = acc + phi[slot, :, cols] * masked[:, cols]
        part = jnp.sum(acc.T, axis=0, keepdims=True)
        rhs_mine[d] = part
        for o in range(1, n):
            rhs_copy(d, o).start()
        rhs_got[d, me] = part
        send_inverse(lax.max(d - ahead, 0), d >= ahead)
        prepare(lax.max(d - 1, 0), 1 - slot)
        pltpu.make_async_copy(inverse.at[0], inv_all.at[d], inv_recv.at[d]).wait()
        first, last = unfold(inv_all[d, 0:LANES, :])
        inv_full[0:LANES, 0:LANES] = first
        inv_full[LANES:, LANES:] = last
        inv_full[LANES:height, 0:LANES] = inv_all[d, LANES:height, :]
        inv_full[0:LANES, LANES:] = inv_full[LANES:, 0:LANES].T
        for o in range(1, n):
            p = peer(me, o, n)
            pltpu.make_async_remote_copy(
                src_ref=rhs_mine.at[d], dst_ref=rhs_got.at[d, p], send_sem=rhs_send.at[d, o],
                recv_sem=rhs_recv.at[d, p], device_id={"path": p}, device_id_type=MESH).wait_recv()
        total = rhs_got[d, 0]
        for p in range(1, n):
            total = total + rhs_got[d, p]
        count = column(stats[2 * rows:2 * rows + 8, :], d)[0:1]
        rhs = total / count
        coef = jnp.sum(inv_full[...] * rhs, axis=1, keepdims=True)
        coefs[...] = jnp.where(lane == d, coef, coefs[...])
        coef_wide = jnp.broadcast_to(coef, (size, LANES))
        parts = []
        for t in range(tiles):
            cols = slice(t * LANES, (t + 1) * LANES)
            parts.append(jnp.sum(phi[slot, :, cols] * coef_wide, axis=0, keepdims=True))
        continuation = jnp.concatenate(parts, axis=1)
        open_date = jnp.where(date_index[...] <= d, money, 0.0)
        weights = jax.nn.sigmoid((exercise - continuation) / temper_scale) * open_date
        flow[...] = value + weights * (exercise - value)
        for o in range(1, n):
            rhs_copy(d, o).wait_send()
        return carry

    lax.fori_loop(0, dates, step, 0)

    final = flow[...]
    part = final[:, 0:LANES]
    for t in range(1, tiles):
        part = part + final[:, t * LANES:(t + 1) * LANES]
    wide = jnp.broadcast_to(part, (8, LANES))
    sum_mine[...] = wide

    def sum_copy(o):
        return pltpu.make_async_remote_copy(
            src_ref=sum_mine, dst_ref=sum_got.at[me], send_sem=sum_send.at[o],
            recv_sem=sum_recv.at[me], device_id={"path": peer(me, o, n)}, device_id_type=MESH)

    for o in range(1, n):
        sum_copy(o).start()
    sum_got[me] = wide
    for o in range(1, n):
        p = peer(me, o, n)
        pltpu.make_async_remote_copy(
            src_ref=sum_mine, dst_ref=sum_got.at[p], send_sem=sum_send.at[o],
            recv_sem=sum_recv.at[p], device_id={"path": p}, device_id_type=MESH).wait_recv()
    total = sum_got[0]
    for p in range(1, n):
        total = total + sum_got[p]
    price[...] = jnp.sum(total[0:1], axis=1, keepdims=True) / (paths * n)
    for o in range(1, n):
        sum_copy(o).wait_send()
    for e in range(dates):
        @pl.when(me == e % n)
        def _():
            for o in range(1, n):
                inv_copy(e, o).wait_send()


def shards(states, itm_flags, terminal, strike, date_index):
    n = lax.axis_size("path")
    dates, factors, paths = states.shape
    f32 = jnp.float32
    basis = 1 + factors + factors * (factors + 1) // 2
    size = 2 * LANES
    height = round_up(basis, 8)
    assert LANES < basis < size
    slots = -(-dates // n)
    rows = round_up(factors, 8)
    dma = pltpu.SemaphoreType.DMA
    big = 60 << 20

    def params(cid):
        return pltpu.CompilerParams(collective_id=cid, has_side_effects=True, vmem_limit_bytes=big)

    stats = pl.pallas_call(
        functools.partial(stats_kernel, n),
        out_shape=jax.ShapeDtypeStruct((2 * rows + 8, LANES), f32),
        in_specs=[VM, VM], out_specs=VM,
        scratch_shapes=[pltpu.VMEM((LANES, LANES), f32), pltpu.VMEM((round_up(dates, 8), LANES), f32),
                        pltpu.VMEM((n, round_up(dates, 8), LANES), f32), dma((n,)), dma((n,))],
        compiler_params=params(0), name="stats")(states, itm_flags)

    system = pl.pallas_call(
        functools.partial(gram_kernel, n, basis),
        out_shape=jax.ShapeDtypeStruct((slots, size, size), f32),
        in_specs=[VM, VM, VM], out_specs=VM,
        scratch_shapes=[pltpu.VMEM((size, paths), f32), pltpu.VMEM((dates, height, LANES), f32),
                        pltpu.VMEM((n, slots, height, LANES), f32), dma((dates,)), dma((n, slots))],
        compiler_params=params(1), name="gram")(states, itm_flags, stats)

    inverse = pl.pallas_call(
        functools.partial(inverse_kernel, basis),
        out_shape=jax.ShapeDtypeStruct((slots, height, LANES), f32),
        in_specs=[VM], out_specs=VM,
        scratch_shapes=[pltpu.VMEM((slots, size, size), f32)],
        compiler_params=pltpu.CompilerParams(vmem_limit_bytes=big), name="inverse")(system)

    flow, price, coefs = pl.pallas_call(
        functools.partial(backward_kernel, n, min(2, dates)),
        out_shape=(jax.ShapeDtypeStruct((1, paths), f32), jax.ShapeDtypeStruct((1, 1), f32),
                   jax.ShapeDtypeStruct((size, LANES), f32)),
        in_specs=[VM] * 7, out_specs=(VM, VM, VM),
        scratch_shapes=[pltpu.VMEM((2, size, paths), f32), pltpu.VMEM((2, 8, paths), f32),
                        pltpu.VMEM((dates, height, LANES), f32), pltpu.VMEM((size, size), f32),
                        pltpu.VMEM((dates, 1, size), f32), pltpu.VMEM((dates, n, 1, size), f32),
                        pltpu.VMEM((8, LANES), f32), pltpu.VMEM((n, 8, LANES), f32),
                        dma((dates, n)), dma((dates,)), dma((dates, n)), dma((dates, n)),
                        dma((n,)), dma((n,))],
        compiler_params=params(2), name="backward",
    )(states, itm_flags, terminal.reshape(1, paths), strike.reshape(1, 1),
      date_index.reshape(1, paths), stats, inverse)
    return flow.reshape(paths), price.reshape(1), coefs[:basis, :dates].T


def solution(mesh):
    in_specs = (
        P(None, None, ("book", "path")),
        P(None, ("book", "path")),
        P(("book", "path")),
        P("book"),
        P(("book", "path")),
    )
    out_specs = (P(("book", "path")), P("book"), P("book", None))
    return jax.shard_map(shards, mesh=mesh, in_specs=in_specs, out_specs=out_specs, check_vma=False)
```
